8 devices in a mesh: tp: 2 (over z, y), side: 2 (over x), rep: 2 (over core).
Axes of the slice: x: 2, y: 2, z: 1, core: 2. Of those that a mesh axis runs over, the one named last changes fastest.
Arguments:
- w_up: float32 [2, 1, 2048, 11008], P('side', None, ('rep', 'tp'))
- w_down: float32 [2, 1, 11008, 2048], P('side', None, None, ('rep', 'tp'))
- g_up: float32 [2, 1, 2048, 11008], P('side', None, ('rep', 'tp'))
- g_down: float32 [2, 1, 11008, 2048], P('side', None, None, ('rep', 'tp'))
- learn_rate: float32 [2], P('side')
- prompts: bfloat16 [2, 2, 8192, 2048], P('side', 'rep')
Outputs:
- output 1: float32 [2, 1, 2048, 11008], P('side', None, ('rep', 'tp'))
- output 2: float32 [2, 1, 11008, 2048], P('side', None, None, ('rep', 'tp'))
- output 3: bfloat16 [2, 2, 8192, 2048], P('side', 'rep')
All inputs are finite; a program needn't handle non-finite values.
Results may differ from the reference program's by a relative error of at most 0.001.
Values are sent between devices in bfloat16 or wider.
A program may use at most 1 GiB of HBM per device.

```python
import jax
import jax.numpy as jnp
from jax import lax

NUM_LAYERS = 1
MODEL_DIM = 2048
HIDDEN_DIM = 11008
NUM_REPS = 2
NUM_TOKENS = 8192


def setup_inputs(seed: int = 0) -> dict:
    keys = jax.random.split(jax.random.key(seed), 6)
    up_shape = (NUM_LAYERS, MODEL_DIM, HIDDEN_DIM)
    down_shape = (NUM_LAYERS, HIDDEN_DIM, MODEL_DIM)
    up_scale = MODEL_DIM ** -0.5
    down_scale = (2.0 / (HIDDEN_DIM * NUM_LAYERS)) ** 0.5
    w_up = jax.random.normal(keys[0], up_shape, jnp.float32) * up_scale
    w_down = jax.random.normal(keys[1], down_shape, jnp.float32) * down_scale
    g_up = jax.random.normal(keys[2], up_shape, jnp.float32) * up_scale
    g_down = jax.random.normal(keys[3], down_shape, jnp.float32) * down_scale
    rate = jax.random.uniform(keys[4], (1,), jnp.float32, 0.04, 0.2)
    prompts = jax.random.normal(keys[5], (NUM_REPS, NUM_TOKENS, MODEL_DIM), jnp.float32)
    zero_up = jnp.zeros(up_shape, jnp.float32)
    zero_down = jnp.zeros(down_shape, jnp.float32)
    return {
        "w_up": jnp.stack([w_up, zero_up]),
        "w_down": jnp.stack([w_down, zero_down]),
        "g_up": jnp.stack([g_up, zero_up]),
        "g_down": jnp.stack([g_down, zero_down]),
        "learn_rate": jnp.concatenate([rate, jnp.zeros((1,), jnp.float32)]),
        "prompts": jnp.stack([jnp.zeros_like(prompts), prompts]).astype(jnp.bfloat16),
    }


def reference(w_up, w_down, g_up, g_down, learn_rate, prompts):
    rate = learn_rate[0]
    new_up = w_up[0] - rate * g_up[0]
    new_down = w_down[0] - rate * g_down[0]
    cast_up = new_up.astype(jnp.bfloat16)
    cast_down = new_down.astype(jnp.bfloat16)

    def layer_step(hidden, weights):
        up_mat, down_mat = weights
        pre_act = jnp.dot(hidden, up_mat, preferred_element_type=jnp.float32)
        act_up = jax.nn.gelu(pre_act, approximate=True).astype(jnp.bfloat16)
        part_sum = jnp.dot(act_up, down_mat, preferred_element_type=jnp.float32)
        return (hidden.astype(jnp.float32) + part_sum).astype(jnp.bfloat16), None

    def replica_forward(rows):
        return lax.scan(layer_step, rows, (cast_up, cast_down))[0]

    gen_out = lax.map(replica_forward, prompts[1])
    up_out = jnp.stack([new_up, jnp.zeros_like(new_up)])
    down_out = jnp.stack([new_down, jnp.zeros_like(new_down)])
    tok_out = jnp.stack([jnp.zeros_like(gen_out), gen_out])
    return (up_out, down_out, tok_out)
```

```python
import jax
import jax.numpy as jnp
from jax import lax
from jax.sharding import PartitionSpec as P

NUM_CHUNKS = 4
TILE = 256


def solution(mesh):
    up_spec = P("side", None, ("rep", "tp"), None)
    down_spec = P("side", None, None, ("rep", "tp"))
    tok_spec = P("side", "rep", None, None)

    def device_step(w_up, w_down, g_up, g_down, learn_rate, prompts):
        rate = learn_rate[0]
        new_up = w_up - rate * g_up
        new_down = w_down - rate * g_down
        cast_up = new_up[0].astype(jnp.bfloat16)
        cast_down = new_down[0].astype(jnp.bfloat16)
        layers, _, hidden_dim = cast_up.shape
        tiles = hidden_dim // TILE
        edges = [TILE * (tiles * k // NUM_CHUNKS) for k in range(NUM_CHUNKS)] + [hidden_dim]
        tp_size = lax.axis_size("tp")
        rows = prompts.shape[2] // tp_size
        hidden = lax.dynamic_slice_in_dim(prompts[0, 0], lax.axis_index("tp") * rows, rows, 0)
        for layer in range(layers):
            total = hidden.astype(jnp.float32)
            part_sum = None
            for lo, hi in zip(edges[:-1], edges[1:]):
                up = lax.ppermute(cast_up[layer, :, lo:hi], "side", perm=[(0, 1)])
                down = lax.ppermute(cast_down[layer, lo:hi, :], "side", perm=[(0, 1)])
                up_other = lax.ppermute(up, "tp", perm=[(0, 1), (1, 0)])
                down_other = lax.ppermute(down, "tp", perm=[(0, 1), (1, 0)])
                first = lax.axis_index("tp") == 0
                up = jnp.concatenate([jnp.where(first, up, up_other), jnp.where(first, up_other, up)], 0)
                down = jnp.concatenate([jnp.where(first, down, down_other), jnp.where(first, down_other, down)], 1)
                up_other = lax.ppermute(up, "rep", perm=[(0, 1), (1, 0)])
                down_other = lax.ppermute(down, "rep", perm=[(0, 1), (1, 0)])
                first = lax.axis_index("rep") == 0
                up = jnp.concatenate([jnp.where(first, up, up_other), jnp.where(first, up_other, up)], 0)
                down = jnp.concatenate([jnp.where(first, down, down_other), jnp.where(first, down_other, down)], 1)
                pre_act = jnp.dot(hidden, up, preferred_element_type=jnp.float32)
                act_up = jax.nn.gelu(pre_act, approximate=True).astype(jnp.bfloat16)
                part = jnp.dot(act_up, down, preferred_element_type=jnp.float32)
                part_sum = part if part_sum is None else part_sum + part
            hidden = (total + part_sum).astype(jnp.bfloat16)
        other = lax.ppermute(hidden, "tp", perm=[(0, 1), (1, 0)])
        first = lax.axis_index("tp") == 0
        gen_out = jnp.concatenate([jnp.where(first, hidden, other), jnp.where(first, other, hidden)], 0)
        return new_up, new_down, gen_out[None, None]

    return jax.shard_map(
        device_step,
        mesh=mesh,
        in_specs=(up_spec, down_spec, up_spec, down_spec, P("side"), tok_spec),
        out_specs=(up_spec, down_spec, tok_spec),
        check_vma=False,
    )
```
